32 devices in a mesh: rep: 2 (over x), dp: 16 (over y, z, core).
Axes of the slice: x: 2, y: 2, z: 4, core: 2. Of those that a mesh axis runs over, the one named last changes fastest.
Arguments:
- x: bfloat16 [32, 2048, 640], P(('rep', 'dp')), parts along dimension 0
- dy: bfloat16 [32, 2048, 640], P(('rep', 'dp')), parts along dimension 0
- wq: bfloat16 [2, 640, 1536], replicated
- wk: bfloat16 [2, 640, 128], replicated
- wv: bfloat16 [2, 640, 128], replicated
- wo: bfloat16 [2, 1536, 640], replicated
- w_gate: bfloat16 [2, 640, 1536], replicated
- w_up: bfloat16 [2, 640, 1536], replicated
- w_down: bfloat16 [2, 1536, 640], replicated
- m_wq: float32 [2, 640, 1536], replicated
- m_wk: float32 [2, 640, 128], replicated
- m_wv: float32 [2, 640, 128], replicated
- m_wo: float32 [2, 1536, 640], replicated
- m_w_gate: float32 [2, 640, 1536], replicated
- m_w_up: float32 [2, 640, 1536], replicated
- m_w_down: float32 [2, 1536, 640], replicated
- v_wq: float32 [2, 640, 1536], replicated
- v_wk: float32 [2, 640, 128], replicated
- v_wv: float32 [2, 640, 128], replicated
- v_wo: float32 [2, 1536, 640], replicated
- v_w_gate: float32 [2, 640, 1536], replicated
- v_w_up: float32 [2, 640, 1536], replicated
- v_w_down: float32 [2, 1536, 640], replicated
Outputs:
- output 1: bfloat16 [4, 640, 1536], P('rep'), parts along dimension 0
- output 2: bfloat16 [4, 640, 128], P('rep'), parts along dimension 0
- output 3: bfloat16 [4, 640, 128], P('rep'), parts along dimension 0
- output 4: bfloat16 [4, 1536, 640], P('rep'), parts along dimension 0
- output 5: bfloat16 [4, 640, 1536], P('rep'), parts along dimension 0
- output 6: bfloat16 [4, 640, 1536], P('rep'), parts along dimension 0
- output 7: bfloat16 [4, 1536, 640], P('rep'), parts along dimension 0
- output 8: float32 [4, 640, 1536], P('rep'), parts along dimension 0
- output 9: float32 [4, 640, 128], P('rep'), parts along dimension 0
- output 10: float32 [4, 640, 128], P('rep'), parts along dimension 0
- output 11: float32 [4, 1536, 640], P('rep'), parts along dimension 0
- output 12: float32 [4, 640, 1536], P('rep'), parts along dimension 0
- output 13: float32 [4, 640, 1536], P('rep'), parts along dimension 0
- output 14: float32 [4, 1536, 640], P('rep'), parts along dimension 0
- output 15: float32 [4, 640, 1536], P('rep'), parts along dimension 0
- output 16: float32 [4, 640, 128], P('rep'), parts along dimension 0
- output 17: float32 [4, 640, 128], P('rep'), parts along dimension 0
- output 18: float32 [4, 1536, 640], P('rep'), parts along dimension 0
- output 19: float32 [4, 640, 1536], P('rep'), parts along dimension 0
- output 20: float32 [4, 640, 1536], P('rep'), parts along dimension 0
- output 21: float32 [4, 1536, 640], P('rep'), parts along dimension 0
There are 2 independent parts. The reference program is written for one: setup_inputs(seed, part) draws one part's arguments, and reference() takes and returns one part's arrays. A program takes and returns all parts, laid end to end along the dimension named above; an argument that names none is the same for every part.
All inputs are finite; a program needn't handle non-finite values.
Results may differ from the reference program's by a relative error of at most 0.024.
Values are sent between devices in bfloat16 or wider.
A program may use at most 2.5 GiB of HBM per device.

```python
import jax
import jax.numpy as jnp
from jax import lax

SEQUENCES = 16
TOKENS = 2048
D = 640
HEADS = 12
KV_HEADS = 1
HEAD = 128
FF = 1536
LAYERS = 2
THETA = 10000
NAMES = ("wq", "wk", "wv", "wo", "w_gate", "w_up", "w_down")
SHAPES = {
    "wq": (LAYERS, D, HEADS * HEAD),
    "wk": (LAYERS, D, KV_HEADS * HEAD),
    "wv": (LAYERS, D, KV_HEADS * HEAD),
    "wo": (LAYERS, HEADS * HEAD, D),
    "w_gate": (LAYERS, D, FF),
    "w_up": (LAYERS, D, FF),
    "w_down": (LAYERS, FF, D),
}


def bump(key, n, height):
    away = (jnp.arange(n, dtype=jnp.int32) - jax.random.randint(key, (), 0, n, jnp.int32)) % n
    return jnp.where(away < n // 8, height, 1.0)


def together(key, own, strength):
    shared = jax.random.normal(key, own.shape[1:], jnp.float32)
    return (own + strength * shared) * lax.rsqrt(1 + strength * strength)


def setup_inputs(seed: int = 0, part: int = 0) -> dict:
    kx, kdy, ka, kb, kz, kf, kh, kl, *keys = jax.random.split(jax.random.key(seed), 8 + 3 * len(NAMES))
    kx, kdy, ka, kb = (jax.random.fold_in(k, part) for k in (kx, kdy, ka, kb))
    kw, km, kv = (keys[i::3] for i in range(3))
    shape = (SEQUENCES, TOKENS, D)
    much_x, much_dy = jax.random.uniform(kz, (2,), jnp.float32, 0.0, 1.0)
    loud = 2.0 ** jax.random.uniform(jax.random.fold_in(kz, 1), (), jnp.float32, -1.0, 2.0)
    layers = 2.0 ** jax.random.uniform(kl, (LAYERS, 1, 1), jnp.float32, -1.0, 1.0)
    times = {"wq": 1.0, "wk": 1.0, "wv": 2.0, "wo": layers, "w_gate": 1.0, "w_up": bump(kh, FF, 4.0), "w_down": layers}
    x = together(ka, jax.random.normal(kx, shape, jnp.float32), much_x) * bump(kf, D, 4.0)
    dy = together(kb, jax.random.normal(kdy, shape, jnp.float32), much_dy)
    drawn = {"x": x.astype(jnp.bfloat16), "dy": (loud * dy * (SEQUENCES * TOKENS) ** -0.5).astype(jnp.bfloat16)}
    for key, name in zip(kw, NAMES, strict=True):
        drawn[name] = (jax.random.normal(key, SHAPES[name], jnp.float32) * SHAPES[name][1] ** -0.5 * times[name]).astype(jnp.bfloat16)
    for key, name in zip(km, NAMES, strict=True):
        drawn[f"m_{name}"] = 0.1 * jax.random.normal(key, SHAPES[name], jnp.float32)
    for key, name in zip(kv, NAMES, strict=True):
        drawn[f"v_{name}"] = loud * loud * jax.random.uniform(key, SHAPES[name], jnp.float32, 0.2, 0.6)
    return drawn


def matmul(a, w):
    return jnp.dot(a, w, preferred_element_type=jnp.float32).astype(jnp.bfloat16)


def normed(h):
    wide = h.astype(jnp.float32)
    scale = lax.rsqrt(jnp.mean(wide**2, -1, keepdims=True) + 1e-6)
    return (wide * scale).astype(jnp.bfloat16)


def turned(t, theta):
    half = t.shape[-1] // 2
    angle = jnp.arange(t.shape[0], dtype=jnp.float32)[:, None] * theta ** (-jnp.arange(half, dtype=jnp.float32) / half)
    cos, sin = jnp.cos(angle)[:, None], jnp.sin(angle)[:, None]
    a, b = t[..., :half].astype(jnp.float32), t[..., half:].astype(jnp.float32)
    return jnp.concatenate([a * cos - b * sin, b * cos + a * sin], -1).astype(jnp.bfloat16)


def seen_by(q, k, v):
    tokens, kv = q.shape[0], k.shape[1]
    q = q.reshape(tokens, kv, -1, q.shape[-1])
    scores = jnp.einsum("tgsd,ugd->gstu", q.astype(jnp.float32), k.astype(jnp.float32)) * q.shape[-1] ** -0.5
    place = jnp.arange(tokens)
    weights = jax.nn.softmax(jnp.where(place[:, None] >= place, scores, -jnp.inf), -1).astype(jnp.bfloat16)
    return jnp.einsum("gstu,ugd->tgsd", weights.astype(jnp.float32), v.astype(jnp.float32)).astype(jnp.bfloat16).reshape(tokens, -1)


def layer(h, w):
    a = normed(h)
    q, k = (turned(matmul(a, w[name]).reshape(h.shape[0], -1, HEAD), THETA) for name in ("wq", "wk"))
    h = h + matmul(seen_by(q, k, matmul(a, w["wv"]).reshape(h.shape[0], -1, HEAD)), w["wo"])
    b = normed(h)
    gate = jnp.dot(b, w["w_gate"], preferred_element_type=jnp.float32)
    up = jnp.dot(b, w["w_up"], preferred_element_type=jnp.float32)
    return h + matmul((jax.nn.silu(gate) * up).astype(jnp.bfloat16), w["w_down"])


def adamw(w, m, v, g):
    m = 0.9 * m + 0.1 * g
    v = 0.95 * v + 0.05 * g * g
    step = m * lax.rsqrt(v + 1e-8) + 0.1 * w
    return (w - 0.02 * step).astype(jnp.bfloat16), m, v


def stack(weights, h):
    return lax.scan(lambda h, w: (layer(h, w), None), h, weights)[0]


def reference(x, dy, wq, wk, wv, wo, w_gate, w_up, w_down, m_wq, m_wk, m_wv, m_wo, m_w_gate, m_w_up, m_w_down, v_wq, v_wk, v_wv, v_wo, v_w_gate, v_w_up, v_w_down):
    weights = dict(zip(NAMES, (wq, wk, wv, wo, w_gate, w_up, w_down), strict=True))

    def take(so_far, sequence):
        h, by_y = sequence
        _, back = jax.vjp(stack, weights, h)
        by_weights, by_h = back(by_y)
        return jax.tree.map(lambda total, term: total + term.astype(jnp.float32), so_far, by_weights), by_h

    none_yet = {name: jnp.zeros(w.shape, jnp.float32) for name, w in weights.items()}
    by_weights, by_x = lax.scan(take, none_yet, (x, dy))
    gradients = [by_weights[name].astype(jnp.bfloat16).astype(jnp.float32) for name in NAMES]
    first = (m_wq, m_wk, m_wv, m_wo, m_w_gate, m_w_up, m_w_down)
    second = (v_wq, v_wk, v_wv, v_wo, v_w_gate, v_w_up, v_w_down)
    new = [adamw(weights[name].astype(jnp.float32), m, v, g) for name, m, v, g in zip(NAMES, first, second, gradients, strict=True)]
    return tuple(one[which] for which in range(3) for one in new)
```

```python
import functools

import jax
import jax.numpy as jnp
from jax import lax
from jax.experimental import pallas as pl
from jax.experimental.pallas import tpu as pltpu
from jax.sharding import PartitionSpec as P

NEG = -1e30
HIDDEN = 2 * NEG
LOG2E = 1.4426950408889634
HEAD = 128
THETA = 10000
NAMES = ("wq", "wk", "wv", "wo", "w_gate", "w_up", "w_down")
VMEM = 60 * 2**20
low, wide = jnp.bfloat16, jnp.float32


def _dot(a, b, ca=1, cb=0):
    return lax.dot_general(a, b, (((ca,), (cb,)), ((), ())), preferred_element_type=wide)


def _params(semantics=("arbitrary",)):
    return pltpu.CompilerParams(dimension_semantics=semantics, vmem_limit_bytes=VMEM)


def _cost(flops, size, exps=0):
    return pl.CostEstimate(flops=int(flops), bytes_accessed=int(size), transcendentals=int(exps))


def _rows(r, c):
    return pl.BlockSpec((r, c), lambda i: (i, 0))


def _layer(w, number):
    return pl.BlockSpec((None, *w.shape[1:]), lambda i: (number, 0, 0), pipeline_mode=pl.Buffered(1))


def _whole(*shape):
    return pl.BlockSpec(shape, lambda i: (0,) * len(shape), pipeline_mode=pl.Buffered(1))


def _norm(h):
    x = h.astype(wide)
    scale = lax.rsqrt(jnp.mean(x * x, -1, keepdims=True) + 1e-6)
    return x * scale, scale


def _norm_bwd(by, n, scale):
    return scale * (by - n * jnp.mean(by * n, -1, keepdims=True))


def _turn(t, cos, sin):
    t = t.astype(wide)
    return (t * cos + pltpu.roll(t, HEAD // 2, 1) * sin).astype(low)


def _qkv_kernel(h_ref, wq_ref, wk_ref, wv_ref, cos_ref, sin_ref, q_ref, k_ref, v_ref):
    a = _norm(h_ref[...])[0].astype(low)
    cos, sin = cos_ref[...], sin_ref[...]
    for at in range(0, q_ref.shape[1], 2 * HEAD):
        t = _dot(a, wq_ref[:, at : at + 2 * HEAD]).astype(low)
        for n in (0, HEAD):
            q_ref[:, at + n : at + n + HEAD] = _turn(t[:, n : n + HEAD], cos, sin)
    k_ref[...] = _turn(_dot(a, wk_ref[...]).astype(low), cos, sin)
    v_ref[...] = _dot(a, wv_ref[...]).astype(low)


def project(h, wq, wk, wv, cos, sin, number, r=512):
    t, d = h.shape
    cq, ck = wq.shape[2], wk.shape[2]
    return pl.pallas_call(
        _qkv_kernel,
        grid=(t // r,),
        in_specs=[_rows(r, d), _layer(wq, number), _layer(wk, number), _layer(wv, number), _rows(r, HEAD), _rows(r, HEAD)],
        out_specs=[_rows(r, cq), _rows(r, ck), _rows(r, ck)],
        out_shape=[jax.ShapeDtypeStruct((t, c), low) for c in (cq, ck, ck)],
        compiler_params=_params(),
        cost_estimate=_cost(2 * t * d * (cq + 2 * ck), 2 * t * (d + cq + 2 * ck)),
        name="qkv",
    )(h, wq, wk, wv, cos, sin)


def _stack_heads(dst, src, bq):
    for n in range(src.shape[1] // HEAD):
        dst[n * bq : (n + 1) * bq, :] = src[:, n * HEAD : (n + 1) * HEAD]


def _lay(ref, g):
    return jnp.concatenate([ref[n : n + 1, :] for n in range(g)], axis=1)


def _attend_kernel(q_ref, k_ref, v_ref, o_ref, lse_ref, q_s, top_s, mix_s, *, scale, bq, bk, strip):
    g = q_ref.shape[1] // HEAD
    cols = g * bq
    iq = pl.program_id(0)
    e = scale * LOG2E
    pieces = list(range(0, cols, strip))
    _stack_heads(q_s, q_ref, bq)
    top_s[...] = jnp.full(top_s.shape, NEG, wide)
    mix_s[...] = jnp.zeros_like(mix_s)

    def block(start, size, masked):
        here = pl.ds(start, size)
        ones = jnp.ones((8, size), low)
        scores = [_dot(k_ref[here, :], q_s[at : at + strip, :], 1, 1) for at in pieces]
        if masked:
            gap = lax.rem(lax.broadcasted_iota(jnp.int32, (size, strip), 1), bq) - lax.broadcasted_iota(jnp.int32, (size, strip), 0)
            ok = gap >= bq - size
        weights, keeps = [], []
        for at, s in zip(pieces, scores):
            if masked:
                s = jnp.where(ok, s, HIDDEN)
            old = top_s[:, at : at + strip]
            top = jnp.maximum(old, s.max(axis=0, keepdims=True))
            top_s[:, at : at + strip] = top
            weights.append(jnp.exp2((s - top) * e).astype(low))
            keeps.append(jnp.exp2((old - top) * e))
        values = jnp.concatenate([v_ref[here, :].T, ones], axis=0)
        for at, p, keep in zip(pieces, weights, keeps):
            mix_s[:, at : at + strip] = mix_s[:, at : at + strip] * keep + _dot(values, p, 1, 0)

    end = (iq + 1) * bq
    full = lax.div(end - bq, bk)
    lax.fori_loop(0, full, lambda j, _: block(pl.multiple_of(j * bk, bk), bk, False), None)
    left = end - full * bk
    for size in range(bq, bk + 1, bq):
        @pl.when(left == size)
        def _():
            block(pl.multiple_of(full * bk, bk), size, True)

    top, total = top_s[...], mix_s[HEAD : HEAD + 1, :]
    out = (mix_s[:HEAD, :] * (1 / total)).astype(low)
    lse = top * scale + jnp.log(total)
    for n in range(g):
        o_ref[:, n * HEAD : (n + 1) * HEAD] = out[:, n * bq : (n + 1) * bq].T
        lse_ref[n : n + 1, :] = lse[:, n * bq : (n + 1) * bq]
    lse_ref[g:, :] = jnp.zeros((lse_ref.shape[0] - g, bq), wide)


def attend(q, k, v, bq=256, bk=512, strip=512):
    t, c = q.shape
    g = c // HEAD
    cols = g * bq
    stats = pl.BlockSpec((16, bq), lambda i: (0, i))
    return pl.pallas_call(
        functools.partial(_attend_kernel, scale=HEAD**-0.5, bq=bq, bk=bk, strip=strip),
        grid=(t // bq,),
        in_specs=[_rows(bq, c), _whole(t, HEAD), _whole(t, HEAD)],
        out_specs=[_rows(bq, c), stats],
        out_shape=[jax.ShapeDtypeStruct((t, c), low), jax.ShapeDtypeStruct((16, t), wide)],
        scratch_shapes=[pltpu.VMEM((cols, HEAD), low), pltpu.VMEM((1, cols), wide), pltpu.VMEM((HEAD + 8, cols), wide)],
        compiler_params=_params(),
        cost_estimate=_cost(2 * t * t * c, 4 * t * c, g * t * t // 2),
        name="attend",
    )(q, k, v)


def _attend_bwd_kernel(q_ref, k_ref, v_ref, do_ref, lse_ref, delta_ref, dq_ref, dk_ref, dv_ref, q_s, do_s, dq_s, dk_s, dv_s,
                       *, scale, bq, bk, strip):
    g = q_ref.shape[1] // HEAD
    cols = g * bq
    iq = pl.program_id(0)
    e = scale * LOG2E
    pieces = list(range(0, cols, strip))
    _stack_heads(q_s, q_ref, bq)
    _stack_heads(do_s, do_ref, bq)

    @pl.when(iq == 0)
    def _():
        dk_s[...] = jnp.zeros_like(dk_s)
        dv_s[...] = jnp.zeros_like(dv_s)

    dq_s[...] = jnp.zeros_like(dq_s)
    lses = _lay(lse_ref, g) * LOG2E
    deltas = _lay(delta_ref, g)

    def block(start, size, masked):
        here = pl.ds(start, size)
        k, v = k_ref[here, :], v_ref[here, :]
        kt = k.T
        if masked:
            gap = lax.rem(lax.broadcasted_iota(jnp.int32, (size, strip), 1), bq) - lax.broadcasted_iota(jnp.int32, (size, strip), 0)
            ok = gap >= bq - size
        qs = [q_s[at : at + strip, :] for at in pieces]
        dos = [do_s[at : at + strip, :] for at in pieces]
        scores = [_dot(k, x, 1, 1) for x in qs]
        dps = [_dot(v, x, 1, 1) for x in dos]
        for n, at in enumerate(pieces):
            p = jnp.exp2(scores[n] * e - lses[:, at : at + strip])
            if masked:
                p = jnp.where(ok, p, 0.0)
            ds = (p * (dps[n] - deltas[:, at : at + strip])).astype(low)
            dv_s[here, :] += _dot(p.astype(low), dos[n], 1, 0)
            dk_s[here, :] += _dot(ds, qs[n], 1, 0)
            dq_s[:, at : at + strip] += _dot(kt, ds, 1, 0)

    end = (iq + 1) * bq
    full = lax.div(end - bq, bk)
    lax.fori_loop(0, full, lambda j, _: block(pl.multiple_of(j * bk, bk), bk, False), None)
    left = end - full * bk
    for size in range(bq, bk + 1, bq):
        @pl.when(left == size)
        def _():
            block(pl.multiple_of(full * bk, bk), size, True)

    for n in range(g):
        dq_ref[:, n * HEAD : (n + 1) * HEAD] = (dq_s[:, n * bq : (n + 1) * bq] * scale).astype(low).T

    @pl.when(iq == pl.num_programs(0) - 1)
    def _():
        dk_ref[...] = (dk_s[...] * scale).astype(low)
        dv_ref[...] = dv_s[...].astype(low)


def attend_bwd(q, k, v, do, lse, delta, bq=256, bk=256, strip=512):
    t, c = q.shape
    g = c // HEAD
    cols = g * bq
    stats = pl.BlockSpec((16, bq), lambda i: (0, i))
    return pl.pallas_call(
        functools.partial(_attend_bwd_kernel, scale=HEAD**-0.5, bq=bq, bk=bk, strip=strip),
        grid=(t // bq,),
        in_specs=[_rows(bq, c), _whole(t, HEAD), _whole(t, HEAD), _rows(bq, c), stats, stats],
        out_specs=[_rows(bq, c), _whole(t, HEAD), _whole(t, HEAD)],
        out_shape=[jax.ShapeDtypeStruct((t, c), low), jax.ShapeDtypeStruct((t, HEAD), low), jax.ShapeDtypeStruct((t, HEAD), low)],
        scratch_shapes=[pltpu.VMEM((cols, HEAD), low), pltpu.VMEM((cols, HEAD), low), pltpu.VMEM((HEAD, cols), wide),
                        pltpu.VMEM((t, HEAD), wide), pltpu.VMEM((t, HEAD), wide)],
        compiler_params=_params(),
        cost_estimate=_cost(5 * t * t * c, 8 * t * c, g * t * t // 2),
        name="attend_bwd",
    )(q, k, v, do, lse, delta)


CHUNK = 512


def _post_kernel(att_ref, h_ref, wo_ref, wg_ref, wu_ref, wd_ref, h1_ref, h2_ref, act_s):
    h1 = (h_ref[...].astype(wide) + _dot(att_ref[...], wo_ref[...]).astype(low).astype(wide)).astype(low)
    h1_ref[...] = h1
    b = _norm(h1)[0].astype(low)
    for at in range(0, act_s.shape[1], CHUNK):
        gate, up = _dot(b, wg_ref[:, at : at + CHUNK]), _dot(b, wu_ref[:, at : at + CHUNK])
        act_s[:, at : at + CHUNK] = (gate * jax.nn.sigmoid(gate) * up).astype(low)
    h2_ref[...] = (h1.astype(wide) + _dot(act_s[...], wd_ref[...]).astype(low).astype(wide)).astype(low)


def post(att, h, wo, wg, wu, wd, number, r=512):
    t, d = h.shape
    c, f = att.shape[1], wg.shape[2]
    return pl.pallas_call(
        _post_kernel,
        grid=(t // r,),
        in_specs=[_rows(r, c), _rows(r, d)] + [_layer(w, number) for w in (wo, wg, wu, wd)],
        out_specs=[_rows(r, d), _rows(r, d)],
        out_shape=[jax.ShapeDtypeStruct((t, d), low)] * 2,
        scratch_shapes=[pltpu.VMEM((r, f), low)],
        compiler_params=_params(),
        cost_estimate=_cost(2 * t * d * (c + 3 * f), 2 * t * (c + 3 * d)),
        name="post",
    )(att, h, wo, wg, wu, wd)


def _post_bwd_kernel(att_ref, h_ref, by_ref, wo_ref, wg_ref, wu_ref, wd_ref, by1_ref, datt_ref, delta_ref, dwo_ref, dwg_ref, dwu_ref, dwd_ref,
                     dwo_s, dwg_s, dwu_s, dwd_s, *, again):
    i = pl.program_id(0)

    @pl.when(i == 0)
    def _():
        for s in (dwo_s, dwg_s, dwu_s, dwd_s):
            s[...] = jnp.zeros_like(s)

    h1 = h_ref[...]
    if again:
        h1 = (h1.astype(wide) + _dot(att_ref[...], wo_ref[...]).astype(low).astype(wide)).astype(low)
    n, scale = _norm(h1)
    b = n.astype(low)
    bt = b.T
    by = by_ref[...]
    byt = by.T
    db = None
    for at in range(0, wg_ref.shape[1], CHUNK):
        here = slice(at, at + CHUNK)
        gate, up = _dot(b, wg_ref[:, here]), _dot(b, wu_ref[:, here])
        sig = jax.nn.sigmoid(gate)
        silu = gate * sig
        act = (silu * up).astype(low)
        dact = _dot(by, wd_ref[here, :], 1, 1).astype(low).astype(wide)
        dup = (dact * silu).astype(low)
        dgate = (dact * up * (sig * (1.0 + gate * (1.0 - sig)))).astype(low)
        dwd_s[:, here] += _dot(byt, act)
        dwg_s[:, here] += _dot(bt, dgate)
        dwu_s[:, here] += _dot(bt, dup)
        part = _dot(dgate, wg_ref[:, here], 1, 1) + _dot(dup, wu_ref[:, here], 1, 1)
        db = part if db is None else db + part
    by1 = (by.astype(wide) + _norm_bwd(db, n, scale)).astype(low)
    by1_ref[...] = by1
    by1t = by1.T
    lanes = att_ref.shape[1]
    r = by1.shape[0]
    delta = None
    for at in range(0, lanes, CHUNK):
        here = slice(at, at + CHUNK)
        att = att_ref[:, here]
        datt = _dot(by1, wo_ref[here, :], 1, 1).astype(low)
        datt_ref[:, here] = datt
        dwo_s[:, here] += _dot(by1t, att)
        prod = att.astype(wide) * datt.astype(wide)
        high = prod.astype(low)
        rest = (prod - high.astype(wide)).astype(low)
        pick = lax.div(lax.broadcasted_iota(jnp.int32, (16, CHUNK), 1) + at, HEAD) == lax.broadcasted_iota(jnp.int32, (16, CHUNK), 0)
        pick = pick.astype(wide).astype(low)
        part = _dot(pick, high, 1, 1) + _dot(pick, rest, 1, 1)
        delta = part if delta is None else delta + part
    delta_ref[...] = delta

    @pl.when(i == pl.num_programs(0) - 1)
    def _():
        dwg_ref[...] = dwg_s[...].astype(low)
        dwu_ref[...] = dwu_s[...].astype(low)
        for out, s in ((dwo_ref, dwo_s), (dwd_ref, dwd_s)):
            for at in range(0, out.shape[0], 256):
                out[at : at + 256, :] = s[:, at : at + 256].astype(low).T


def post_bwd(att, h, by, wo, wg, wu, wd, number, again, r=512):
    t, d = h.shape
    c, f = att.shape[1], wg.shape[2]
    return pl.pallas_call(
        functools.partial(_post_bwd_kernel, again=again),
        grid=(t // r,),
        in_specs=[_rows(r, c), _rows(r, d), _rows(r, d)] + [_layer(w, number) for w in (wo, wg, wu, wd)],
        out_specs=[_rows(r, d), _rows(r, c), pl.BlockSpec((16, r), lambda i: (0, i)), _whole(c, d), _whole(d, f), _whole(d, f), _whole(f, d)],
        out_shape=[jax.ShapeDtypeStruct((t, d), low), jax.ShapeDtypeStruct((t, c), low), jax.ShapeDtypeStruct((16, t), wide),
                   jax.ShapeDtypeStruct((c, d), low), jax.ShapeDtypeStruct((d, f), low), jax.ShapeDtypeStruct((d, f), low),
                   jax.ShapeDtypeStruct((f, d), low)],
        scratch_shapes=[pltpu.VMEM((d, c), wide), pltpu.VMEM((d, f), wide), pltpu.VMEM((d, f), wide), pltpu.VMEM((d, f), wide)],
        compiler_params=_params(),
        cost_estimate=_cost(2 * t * d * (3 * c + 8 * f), 2 * t * (2 * c + 3 * d)),
        name="post_bwd",
    )(att, h, by, wo, wg, wu, wd)


def _qkv_bwd_kernel(dq_ref, dk_ref, dv_ref, h_ref, cos_ref, sin_ref, *rest, deep):
    if deep:
        by1_ref, wq_ref, wk_ref, wv_ref, dwq_ref, dwk_ref, dwv_ref, by_ref, dwq_s, dwkv_s = rest
    else:
        dwq_ref, dwk_ref, dwv_ref, dwq_s, dwkv_s = rest
    i = pl.program_id(0)

    @pl.when(i == 0)
    def _():
        dwq_s[...] = jnp.zeros_like(dwq_s)
        dwkv_s[...] = jnp.zeros_like(dwkv_s)

    n, scale = _norm(h_ref[...])
    at_ = n.astype(low).T
    cos, sin = cos_ref[...], -sin_ref[...]
    dk = _turn(dk_ref[...], cos, sin)
    dv = dv_ref[...]
    dkv = jnp.concatenate([dk, dv], axis=1)
    dwkv_s[...] += _dot(at_, dkv)
    da = _dot(dk, wk_ref[...], 1, 1) + _dot(dv, wv_ref[...], 1, 1) if deep else None
    for at in range(0, dq_ref.shape[1], CHUNK):
        here = slice(at, at + CHUNK)
        dq = jnp.concatenate([_turn(dq_ref[:, at + x : at + x + HEAD], cos, sin) for x in range(0, CHUNK, HEAD)], axis=1)
        dwq_s[:, here] += _dot(at_, dq)
        if deep:
            da += _dot(dq, wq_ref[:, here], 1, 1)
    if deep:
        by_ref[...] = (by1_ref[...].astype(wide) + _norm_bwd(da, n, scale)).astype(low)

    @pl.when(i == pl.num_programs(0) - 1)
    def _():
        dwq_ref[...] = dwq_s[...].astype(low)
        dwk_ref[...] = dwkv_s[:, :HEAD].astype(low)
        dwv_ref[...] = dwkv_s[:, HEAD:].astype(low)


def project_bwd(dq, dk, dv, h, cos, sin, number, deep, by1=None, wq=None, wk=None, wv=None, r=512):
    t, d = h.shape
    c = dq.shape[1]
    ins, specs = [dq, dk, dv, h, cos, sin], [_rows(r, c), _rows(r, HEAD), _rows(r, HEAD), _rows(r, d), _rows(r, HEAD), _rows(r, HEAD)]
    outs = [jax.ShapeDtypeStruct((d, c), low), jax.ShapeDtypeStruct((d, HEAD), low), jax.ShapeDtypeStruct((d, HEAD), low)]
    out_specs = [_whole(d, c), _whole(d, HEAD), _whole(d, HEAD)]
    if deep:
        ins += [by1, wq, wk, wv]
        specs += [_rows(r, d)] + [_layer(w, number) for w in (wq, wk, wv)]
        outs += [jax.ShapeDtypeStruct((t, d), low)]
        out_specs += [_rows(r, d)]
    return pl.pallas_call(
        functools.partial(_qkv_bwd_kernel, deep=deep),
        grid=(t // r,),
        in_specs=specs,
        out_specs=out_specs,
        out_shape=outs,
        scratch_shapes=[pltpu.VMEM((d, c), wide), pltpu.VMEM((d, 2 * HEAD), wide)],
        compiler_params=_params(),
        cost_estimate=_cost(2 * t * d * (c + 2 * HEAD) * (2 if deep else 1), 2 * t * (c + 3 * d)),
        name="qkv_bwd",
    )(*ins)


def _adamw_kernel(*refs, count, kept):
    ins, outs = refs[: 4 * count], refs[4 * count + kept :]
    for n in range(count):
        w_ref, m_ref, v_ref, g_ref = ins[4 * n : 4 * n + 4]
        g = g_ref[...].astype(wide)
        w = w_ref[...].astype(wide)
        m = 0.9 * m_ref[...] + 0.1 * g
        v = 0.95 * v_ref[...] + 0.05 * g * g
        outs[3 * n][...] = (w - 0.02 * (m * lax.rsqrt(v + 1e-8) + 0.1 * w)).astype(low)
        outs[3 * n + 1][...] = m
        outs[3 * n + 2][...] = v


def adamw(items, state, new, steps=8):
    ins, specs, shapes, out_specs, keep, alias = [], [], [], [], [], {}
    for name, number, g in items:
        w, m, v = state[name]
        rows, cols = w.shape[1:]
        r = rows // steps
        spec = pl.BlockSpec((None, r, cols), functools.partial(lambda number, i: (number, i, 0), number))
        ins += [w, m, v, g]
        specs += [spec, spec, spec, pl.BlockSpec((r, cols), lambda i: (i, 0))]
        for one in (w, m, v):
            shapes.append(jax.ShapeDtypeStruct(one.shape, one.dtype))
            out_specs.append(spec)
    for n, (name, _, _) in enumerate(items):
        if name in new:
            for x in range(3):
                alias[len(ins) + len(keep)] = 3 * n + x
                keep.append(new[name][x])
    got = pl.pallas_call(
        functools.partial(_adamw_kernel, count=len(items), kept=len(keep)),
        grid=(steps,),
        in_specs=specs + [pl.BlockSpec(memory_space=pl.ANY)] * len(keep),
        out_specs=out_specs,
        out_shape=shapes,
        input_output_aliases=alias,
        compiler_params=_params(),
        cost_estimate=_cost(sum(2000 * g.size for _, _, g in items), sum(22 * g.size for _, _, g in items)),
        name="adamw",
    )(*ins, *keep)
    for n, (name, _, _) in enumerate(items):
        new[name] = got[3 * n : 3 * n + 3]


def reduced(grads, after=None):
    grads = tuple(grads)
    if after is not None:
        grads, _ = lax.optimization_barrier((grads, after))
    return lax.psum(grads, "dp")


def solution(mesh):
    def step(x, dy, *arrays):
        weights, m, v = (arrays[i : i + 7] for i in (0, 7, 14))
        state = {name: one for name, *one in zip(NAMES, weights, m, v, strict=True)}
        wq, wk, wv, wo, wg, wu, wd = weights
        layers = wq.shape[0]
        h, by = x[0], dy[0]
        t = h.shape[0]
        half = HEAD // 2
        angle = jnp.arange(t, dtype=wide)[:, None] * THETA ** (-jnp.arange(half, dtype=wide) / half)
        cos, sin = jnp.cos(angle), jnp.sin(angle)
        cos, sin = jnp.concatenate([cos, cos], 1), jnp.concatenate([-sin, sin], 1)
        kept = []
        for n in range(layers):
            q, k, val = project(h, wq, wk, wv, cos, sin, n)
            att, lse = attend(q, k, val)
            if n < layers - 1:
                h1, h2 = post(att, h, wo, wg, wu, wd, n)
                kept.append((h, q, k, val, att, lse, h1))
                h = h2
            else:
                kept.append((h, q, k, val, att, lse, h))
        new, first, last_sum, waiting, done = {}, [], None, [], []
        for n in reversed(range(layers)):
            h, q, k, val, att, lse, h1 = kept[n]
            by1, datt, delta, dwo, dwg, dwu, dwd = post_bwd(att, h1, by, wo, wg, wu, wd, n, n == layers - 1)
            waiting += [("wo", n, dwo), ("w_gate", n, dwg), ("w_up", n, dwu), ("w_down", n, dwd)]
            got = reduced([g for _, _, g in waiting], last_sum)
            done.append([(name, at, g) for (name, at, _), g in zip(waiting, got)])
            last_sum = got
            dq, dk, dv = attend_bwd(q, k, val, datt, lse, delta)
            dwq, dwk, dwv, *by = project_bwd(dq, dk, dv, h, cos, sin, n, n > 0, by1, wq, wk, wv)
            by = by[0] if by else None
            waiting = [("wq", n, dwq), ("wk", n, dwk), ("wv", n, dwv)]
        got = reduced([g for _, _, g in waiting], last_sum)
        done.append([(name, at, g) for (name, at, _), g in zip(waiting, got)])
        for items in done:
            adamw(items, state, new)
        return tuple(new[name][which] for which in range(3) for name in NAMES)

    states, all_of = P(("rep", "dp"), None, None), P(None, None, None)
    return jax.shard_map(
        step,
        mesh=mesh,
        in_specs=(states, states) + (all_of,) * 21,
        out_specs=(P("rep", None, None),) * 21,
        check_vma=False,
    )
```

```python
import functools

import jax
import jax.numpy as jnp
from jax import lax
from jax.experimental import pallas as pl
from jax.experimental.pallas import tpu as pltpu
from jax.sharding import PartitionSpec as P


NEG = -1e30
HIDDEN = 2 * NEG
LOG2E = 1.4426950408889634
HEAD = 128
THETA = 10000
NAMES = ("wq", "wk", "wv", "wo", "w_gate", "w_up", "w_down")
VMEM = 60 * 2**20
low, wide = jnp.bfloat16, jnp.float32


def _dot(a, b, ca=1, cb=0):
    return lax.dot_general(a, b, (((ca,), (cb,)), ((), ())), preferred_element_type=wide)


def _params(semantics=("arbitrary",)):
    return pltpu.CompilerParams(dimension_semantics=semantics, vmem_limit_bytes=VMEM)


def _cost(flops, size, exps=0):
    return pl.CostEstimate(flops=int(flops), bytes_accessed=int(size), transcendentals=int(exps))


def _rows(r, c):
    return pl.BlockSpec((r, c), lambda i: (i, 0))


def _layer(w, number):
    return pl.BlockSpec((None, *w.shape[1:]), lambda i: (number, 0, 0), pipeline_mode=pl.Buffered(1))


def _whole(*shape):
    return pl.BlockSpec(shape, lambda i: (0,) * len(shape), pipeline_mode=pl.Buffered(1))


def _norm(h):
    x = h.astype(wide)
    scale = lax.rsqrt(jnp.mean(x * x, -1, keepdims=True) + 1e-6)
    return x * scale, scale


def _norm_bwd(by, n, scale):
    return scale * (by - n * jnp.mean(by * n, -1, keepdims=True))


def _turn(t, cos, sin):
    t = t.astype(wide)
    return (t * cos + pltpu.roll(t, HEAD // 2, 1) * sin).astype(low)


def _late(kernel, at, count):
    return lambda *refs: kernel(*refs[:at], *refs[at + count :])


def _qkv_kernel(h_ref, wq_ref, wk_ref, wv_ref, cos_ref, sin_ref, q_ref, k_ref, v_ref):
    a = _norm(h_ref[...])[0].astype(low)
    cos, sin = cos_ref[...], sin_ref[...]
    for at in range(0, q_ref.shape[1], 2 * HEAD):
        t = _dot(a, wq_ref[:, at : at + 2 * HEAD]).astype(low)
        for n in (0, HEAD):
            q_ref[:, at + n : at + n + HEAD] = _turn(t[:, n : n + HEAD], cos, sin)
    k_ref[...] = _turn(_dot(a, wk_ref[...]).astype(low), cos, sin)
    v_ref[...] = _dot(a, wv_ref[...]).astype(low)


def project(h, wq, wk, wv, cos, sin, number, r=512):
    t, d = h.shape
    cq, ck = wq.shape[2], wk.shape[2]
    return pl.pallas_call(
        _qkv_kernel,
        grid=(t // r,),
        in_specs=[_rows(r, d), _layer(wq, number), _layer(wk, number), _layer(wv, number), _rows(r, HEAD), _rows(r, HEAD)],
        out_specs=[_rows(r, cq), _rows(r, ck), _rows(r, ck)],
        out_shape=[jax.ShapeDtypeStruct((t, c), low) for c in (cq, ck, ck)],
        compiler_params=_params(),
        cost_estimate=_cost(2 * t * d * (cq + 2 * ck), 2 * t * (d + cq + 2 * ck)),
        name="qkv",
    )(h, wq, wk, wv, cos, sin)


def _stack_heads(dst, src, bq):
    for n in range(src.shape[1] // HEAD):
        dst[n * bq : (n + 1) * bq, :] = src[:, n * HEAD : (n + 1) * HEAD]


def _lay(ref, g):
    return jnp.concatenate([ref[n : n + 1, :] for n in range(g)], axis=1)


def _attend_kernel(q_ref, k_ref, v_ref, o_ref, lse_ref, q_s, top_s, mix_s, *, scale, bq, bk, strip):
    g = q_ref.shape[1] // HEAD
    cols = g * bq
    iq = pl.program_id(0)
    e = scale * LOG2E
    pieces = list(range(0, cols, strip))
    _stack_heads(q_s, q_ref, bq)
    top_s[...] = jnp.full(top_s.shape, NEG, wide)
    mix_s[...] = jnp.zeros_like(mix_s)

    def block(start, size, masked):
        here = pl.ds(start, size)
        ones = jnp.ones((8, size), low)
        scores = [_dot(k_ref[here, :], q_s[at : at + strip, :], 1, 1) for at in pieces]
        if masked:
            gap = lax.rem(lax.broadcasted_iota(jnp.int32, (size, strip), 1), bq) - lax.broadcasted_iota(jnp.int32, (size, strip), 0)
            ok = gap >= bq - size
        weights, keeps = [], []
        for at, s in zip(pieces, scores):
            if masked:
                s = jnp.where(ok, s, HIDDEN)
            old = top_s[:, at : at + strip]
            top = jnp.maximum(old, s.max(axis=0, keepdims=True))
            top_s[:, at : at + strip] = top
            weights.append(jnp.exp2((s - top) * e).astype(low))
            keeps.append(jnp.exp2((old - top) * e))
        values = jnp.concatenate([v_ref[here, :].T, ones], axis=0)
        for at, p, keep in zip(pieces, weights, keeps):
            mix_s[:, at : at + strip] = mix_s[:, at : at + strip] * keep + _dot(values, p, 1, 0)

    end = (iq + 1) * bq
    full = lax.div(end - bq, bk)
    lax.fori_loop(0, full, lambda j, _: block(pl.multiple_of(j * bk, bk), bk, False), None)
    left = end - full * bk
    for size in range(bq, bk + 1, bq):
        @pl.when(left == size)
        def _():
            block(pl.multiple_of(full * bk, bk), size, True)

    top, total = top_s[...], mix_s[HEAD : HEAD + 1, :]
    out = (mix_s[:HEAD, :] * (1 / total)).astype(low)
    lse = top * scale + jnp.log(total)
    for n in range(g):
        o_ref[:, n * HEAD : (n + 1) * HEAD] = out[:, n * bq : (n + 1) * bq].T
        lse_ref[n : n + 1, :] = lse[:, n * bq : (n + 1) * bq]
    lse_ref[g:, :] = jnp.zeros((lse_ref.shape[0] - g, bq), wide)


def attend(q, k, v, bq=256, bk=512, strip=512):
    t, c = q.shape
    g = c // HEAD
    cols = g * bq
    stats = pl.BlockSpec((16, bq), lambda i: (0, i))
    return pl.pallas_call(
        functools.partial(_attend_kernel, scale=HEAD**-0.5, bq=bq, bk=bk, strip=strip),
        grid=(t // bq,),
        in_specs=[_rows(bq, c), _whole(t, HEAD), _whole(t, HEAD)],
        out_specs=[_rows(bq, c), stats],
        out_shape=[jax.ShapeDtypeStruct((t, c), low), jax.ShapeDtypeStruct((16, t), wide)],
        scratch_shapes=[pltpu.VMEM((cols, HEAD), low), pltpu.VMEM((1, cols), wide), pltpu.VMEM((HEAD + 8, cols), wide)],
        compiler_params=_params(),
        cost_estimate=_cost(2 * t * t * c, 4 * t * c, g * t * t // 2),
        name="attend",
    )(q, k, v)


def _attend_bwd_kernel(q_ref, k_ref, v_ref, do_ref, lse_ref, delta_ref, dq_ref, dk_ref, dv_ref, q_s, do_s, dq_s, dk_s, dv_s,
                       *, scale, bq, bk, strip):
    g = q_ref.shape[1] // HEAD
    cols = g * bq
    iq = pl.program_id(0)
    e = scale * LOG2E
    pieces = list(range(0, cols, strip))
    _stack_heads(q_s, q_ref, bq)
    _stack_heads(do_s, do_ref, bq)

    @pl.when(iq == 0)
    def _():
        dk_s[...] = jnp.zeros_like(dk_s)
        dv_s[...] = jnp.zeros_like(dv_s)

    dq_s[...] = jnp.zeros_like(dq_s)
    lses = _lay(lse_ref, g) * LOG2E
    deltas = _lay(delta_ref, g)

    def block(start, size, masked):
        here = pl.ds(start, size)
        k, v = k_ref[here, :], v_ref[here, :]
        kt = k.T
        if masked:
            gap = lax.rem(lax.broadcasted_iota(jnp.int32, (size, strip), 1), bq) - lax.broadcasted_iota(jnp.int32, (size, strip), 0)
            ok = gap >= bq - size
        qs = [q_s[at : at + strip, :] for at in pieces]
        dos = [do_s[at : at + strip, :] for at in pieces]
        scores = [_dot(k, x, 1, 1) for x in qs]
        dps = [_dot(v, x, 1, 1) for x in dos]
        for n, at in enumerate(pieces):
            p = jnp.exp2(scores[n] * e - lses[:, at : at + strip])
            if masked:
                p = jnp.where(ok, p, 0.0)
            ds = (p * (dps[n] - deltas[:, at : at + strip])).astype(low)
            dv_s[here, :] += _dot(p.astype(low), dos[n], 1, 0)
            dk_s[here, :] += _dot(ds, qs[n], 1, 0)
            dq_s[:, at : at + strip] += _dot(kt, ds, 1, 0)

    end = (iq + 1) * bq
    full = lax.div(end - bq, bk)
    lax.fori_loop(0, full, lambda j, _: block(pl.multiple_of(j * bk, bk), bk, False), None)
    left = end - full * bk
    for size in range(bq, bk + 1, bq):
        @pl.when(left == size)
        def _():
            block(pl.multiple_of(full * bk, bk), size, True)

    for n in range(g):
        dq_ref[:, n * HEAD : (n + 1) * HEAD] = (dq_s[:, n * bq : (n + 1) * bq] * scale).astype(low).T

    @pl.when(iq == pl.num_programs(0) - 1)
    def _():
        dk_ref[...] = (dk_s[...] * scale).astype(low)
        dv_ref[...] = dv_s[...].astype(low)


def attend_bwd(q, k, v, do, lse, delta, after=(), bq=256, bk=256, strip=512):
    t, c = q.shape
    g = c // HEAD
    cols = g * bq
    stats = pl.BlockSpec((16, bq), lambda i: (0, i))
    return pl.pallas_call(
        _late(functools.partial(_attend_bwd_kernel, scale=HEAD**-0.5, bq=bq, bk=bk, strip=strip), 6, len(after)),
        grid=(t // bq,),
        in_specs=[_rows(bq, c), _whole(t, HEAD), _whole(t, HEAD), _rows(bq, c), stats, stats] + [pl.BlockSpec(memory_space=pl.ANY)] * len(after),
        out_specs=[_rows(bq, c), _whole(t, HEAD), _whole(t, HEAD)],
        out_shape=[jax.ShapeDtypeStruct((t, c), low), jax.ShapeDtypeStruct((t, HEAD), low), jax.ShapeDtypeStruct((t, HEAD), low)],
        scratch_shapes=[pltpu.VMEM((cols, HEAD), low), pltpu.VMEM((cols, HEAD), low), pltpu.VMEM((HEAD, cols), wide),
                        pltpu.VMEM((t, HEAD), wide), pltpu.VMEM((t, HEAD), wide)],
        compiler_params=_params(),
        cost_estimate=_cost(5 * t * t * c, 8 * t * c, g * t * t // 2),
        name="attend_bwd",
    )(q, k, v, do, lse, delta, *after)


CHUNK = 512


def _post_kernel(att_ref, h_ref, wo_ref, wg_ref, wu_ref, wd_ref, h1_ref, h2_ref, act_s):
    h1 = (h_ref[...].astype(wide) + _dot(att_ref[...], wo_ref[...]).astype(low).astype(wide)).astype(low)
    h1_ref[...] = h1
    b = _norm(h1)[0].astype(low)
    for at in range(0, act_s.shape[1], CHUNK):
        gate, up = _dot(b, wg_ref[:, at : at + CHUNK]), _dot(b, wu_ref[:, at : at + CHUNK])
        act_s[:, at : at + CHUNK] = (gate * jax.nn.sigmoid(gate) * up).astype(low)
    h2_ref[...] = (h1.astype(wide) + _dot(act_s[...], wd_ref[...]).astype(low).astype(wide)).astype(low)


def post(att, h, wo, wg, wu, wd, number, r=512):
    t, d = h.shape
    c, f = att.shape[1], wg.shape[2]
    return pl.pallas_call(
        _post_kernel,
        grid=(t // r,),
        in_specs=[_rows(r, c), _rows(r, d)] + [_layer(w, number) for w in (wo, wg, wu, wd)],
        out_specs=[_rows(r, d), _rows(r, d)],
        out_shape=[jax.ShapeDtypeStruct((t, d), low)] * 2,
        scratch_shapes=[pltpu.VMEM((r, f), low)],
        compiler_params=_params(),
        cost_estimate=_cost(2 * t * d * (c + 3 * f), 2 * t * (c + 3 * d)),
        name="post",
    )(att, h, wo, wg, wu, wd)


def _post_bwd_kernel(att_ref, h_ref, by_ref, wo_ref, wg_ref, wu_ref, wd_ref, by1_ref, datt_ref, delta_ref, dwo_ref, dwg_ref, dwu_ref, dwd_ref,
                     dwo_s, dwg_s, dwu_s, dwd_s, *, again):
    i = pl.program_id(0)

    @pl.when(i == 0)
    def _():
        for s in (dwo_s, dwg_s, dwu_s, dwd_s):
            s[...] = jnp.zeros_like(s)

    h1 = h_ref[...]
    if again:
        h1 = (h1.astype(wide) + _dot(att_ref[...], wo_ref[...]).astype(low).astype(wide)).astype(low)
    n, scale = _norm(h1)
    b = n.astype(low)
    bt = b.T
    by = by_ref[...]
    byt = by.T
    db = None
    for at in range(0, wg_ref.shape[1], CHUNK):
        here = slice(at, at + CHUNK)
        gate, up = _dot(b, wg_ref[:, here]), _dot(b, wu_ref[:, here])
        sig = jax.nn.sigmoid(gate)
        silu = gate * sig
        act = (silu * up).astype(low)
        dact = _dot(by, wd_ref[here, :], 1, 1).astype(low).astype(wide)
        dup = (dact * silu).astype(low)
        dgate = (dact * up * (sig * (1.0 + gate * (1.0 - sig)))).astype(low)
        dwd_s[:, here] += _dot(byt, act)
        dwg_s[:, here] += _dot(bt, dgate)
        dwu_s[:, here] += _dot(bt, dup)
        part = _dot(dgate, wg_ref[:, here], 1, 1) + _dot(dup, wu_ref[:, here], 1, 1)
        db = part if db is None else db + part
    by1 = (by.astype(wide) + _norm_bwd(db, n, scale)).astype(low)
    by1_ref[...] = by1
    by1t = by1.T
    lanes = att_ref.shape[1]
    r = by1.shape[0]
    delta = None
    for at in range(0, lanes, CHUNK):
        here = slice(at, at + CHUNK)
        att = att_ref[:, here]
        datt = _dot(by1, wo_ref[here, :], 1, 1).astype(low)
        datt_ref[:, here] = datt
        dwo_s[:, here] += _dot(by1t, att)
        prod = att.astype(wide) * datt.astype(wide)
        high = prod.astype(low)
        rest = (prod - high.astype(wide)).astype(low)
        pick = lax.div(lax.broadcasted_iota(jnp.int32, (16, CHUNK), 1) + at, HEAD) == lax.broadcasted_iota(jnp.int32, (16, CHUNK), 0)
        pick = pick.astype(wide).astype(low)
        part = _dot(pick, high, 1, 1) + _dot(pick, rest, 1, 1)
        delta = part if delta is None else delta + part
    delta_ref[...] = delta

    @pl.when(i == pl.num_programs(0) - 1)
    def _():
        dwg_ref[...] = dwg_s[...].astype(low)
        dwu_ref[...] = dwu_s[...].astype(low)
        for out, s in ((dwo_ref, dwo_s), (dwd_ref, dwd_s)):
            for at in range(0, out.shape[0], 256):
                out[at : at + 256, :] = s[:, at : at + 256].astype(low).T


def post_bwd(att, h, by, wo, wg, wu, wd, number, again, after=(), r=512):
    t, d = h.shape
    c, f = att.shape[1], wg.shape[2]
    return pl.pallas_call(
        _late(functools.partial(_post_bwd_kernel, again=again), 7, len(after)),
        grid=(t // r,),
        in_specs=[_rows(r, c), _rows(r, d), _rows(r, d)] + [_layer(w, number) for w in (wo, wg, wu, wd)] + [pl.BlockSpec(memory_space=pl.ANY)] * len(after),
        out_specs=[_rows(r, d), _rows(r, c), pl.BlockSpec((16, r), lambda i: (0, i)), _whole(c, d), _whole(d, f), _whole(d, f), _whole(f, d)],
        out_shape=[jax.ShapeDtypeStruct((t, d), low), jax.ShapeDtypeStruct((t, c), low), jax.ShapeDtypeStruct((16, t), wide),
                   jax.ShapeDtypeStruct((c, d), low), jax.ShapeDtypeStruct((d, f), low), jax.ShapeDtypeStruct((d, f), low),
                   jax.ShapeDtypeStruct((f, d), low)],
        scratch_shapes=[pltpu.VMEM((d, c), wide), pltpu.VMEM((d, f), wide), pltpu.VMEM((d, f), wide), pltpu.VMEM((d, f), wide)],
        compiler_params=_params(),
        cost_estimate=_cost(2 * t * d * (3 * c + 8 * f), 2 * t * (2 * c + 3 * d)),
        name="post_bwd",
    )(att, h, by, wo, wg, wu, wd, *after)


def _qkv_bwd_kernel(dq_ref, dk_ref, dv_ref, h_ref, cos_ref, sin_ref, *rest, deep):
    if deep:
        by1_ref, wq_ref, wk_ref, wv_ref, dw_ref, by_ref, dwq_s, dwkv_s = rest
    else:
        dw_ref, dwq_s, dwkv_s = rest
    i = pl.program_id(0)

    @pl.when(i == 0)
    def _():
        dwq_s[...] = jnp.zeros_like(dwq_s)
        dwkv_s[...] = jnp.zeros_like(dwkv_s)

    n, scale = _norm(h_ref[...])
    at_ = n.astype(low).T
    cos, sin = cos_ref[...], -sin_ref[...]
    dk = _turn(dk_ref[...], cos, sin)
    dv = dv_ref[...]
    dkv = jnp.concatenate([dk, dv], axis=1)
    dwkv_s[...] += _dot(at_, dkv)
    da = _dot(dk, wk_ref[...], 1, 1) + _dot(dv, wv_ref[...], 1, 1) if deep else None
    for at in range(0, dq_ref.shape[1], CHUNK):
        here = slice(at, at + CHUNK)
        dq = jnp.concatenate([_turn(dq_ref[:, at + x : at + x + HEAD], cos, sin) for x in range(0, CHUNK, HEAD)], axis=1)
        dwq_s[:, here] += _dot(at_, dq)
        if deep:
            da += _dot(dq, wq_ref[:, here], 1, 1)
    if deep:
        by_ref[...] = (by1_ref[...].astype(wide) + _norm_bwd(da, n, scale)).astype(low)

    @pl.when(i == pl.num_programs(0) - 1)
    def _():
        dw_ref[:, : dwq_s.shape[1]] = dwq_s[...].astype(low)
        dw_ref[:, dwq_s.shape[1] :] = dwkv_s[...].astype(low)


def project_bwd(dq, dk, dv, h, cos, sin, number, deep, by1=None, wq=None, wk=None, wv=None, after=(), r=512):
    t, d = h.shape
    c = dq.shape[1]
    ins, specs = [dq, dk, dv, h, cos, sin], [_rows(r, c), _rows(r, HEAD), _rows(r, HEAD), _rows(r, d), _rows(r, HEAD), _rows(r, HEAD)]
    outs = [jax.ShapeDtypeStruct((d, c + 2 * HEAD), low)]
    out_specs = [_whole(d, c + 2 * HEAD)]
    if deep:
        ins += [by1, wq, wk, wv]
        specs += [_rows(r, d)] + [_layer(w, number) for w in (wq, wk, wv)]
        outs += [jax.ShapeDtypeStruct((t, d), low)]
        out_specs += [_rows(r, d)]
    return pl.pallas_call(
        _late(functools.partial(_qkv_bwd_kernel, deep=deep), len(ins), len(after)),
        grid=(t // r,),
        in_specs=specs + [pl.BlockSpec(memory_space=pl.ANY)] * len(after),
        out_specs=out_specs,
        out_shape=outs,
        scratch_shapes=[pltpu.VMEM((d, c), wide), pltpu.VMEM((d, 2 * HEAD), wide)],
        compiler_params=_params(),
        cost_estimate=_cost(2 * t * d * (c + 2 * HEAD) * (2 if deep else 1), 2 * t * (c + 3 * d)),
        name="qkv_bwd",
    )(*ins, *after)


def _adamw_kernel(*refs, count, kept):
    ins, outs = refs[: 4 * count], refs[4 * count + kept :]
    outs[-1][...] = jnp.zeros_like(outs[-1])
    for n in range(count):
        w_ref, m_ref, v_ref, g_ref = ins[4 * n : 4 * n + 4]
        g = g_ref[...].astype(wide)
        w = w_ref[...].astype(wide)
        m = 0.9 * m_ref[...] + 0.1 * g
        v = 0.95 * v_ref[...] + 0.05 * g * g
        outs[3 * n][...] = (w - 0.02 * (m * lax.rsqrt(v + 1e-8) + 0.1 * w)).astype(low)
        outs[3 * n + 1][...] = m
        outs[3 * n + 2][...] = v


def adamw(items, state, new, after=(), steps=8):
    ins, specs, shapes, out_specs, keep, alias = [], [], [], [], [], {}
    for name, number, g in items:
        w, m, v = state[name]
        rows, cols = w.shape[1:]
        r = rows // steps
        spec = pl.BlockSpec((None, r, cols), functools.partial(lambda number, i: (number, i, 0), number))
        ins += [w, m, v, g]
        specs += [spec, spec, spec, pl.BlockSpec((r, cols), lambda i: (i, 0))]
        for one in (w, m, v):
            shapes.append(jax.ShapeDtypeStruct(one.shape, one.dtype))
            out_specs.append(spec)
    for n, (name, _, _) in enumerate(items):
        if name in new:
            for x in range(3):
                alias[len(ins) + len(keep)] = 3 * n + x
                keep.append(new[name][x])
    got = pl.pallas_call(
        functools.partial(_adamw_kernel, count=len(items), kept=len(keep) + len(after)),
        grid=(steps,),
        in_specs=specs + [pl.BlockSpec(memory_space=pl.ANY)] * (len(keep) + len(after)),
        out_specs=out_specs + [pl.BlockSpec((8, HEAD), lambda i: (0, 0))],
        out_shape=shapes + [jax.ShapeDtypeStruct((8, HEAD), wide)],
        input_output_aliases=alias,
        compiler_params=_params(),
        cost_estimate=_cost(sum(2000 * g.size for _, _, g in items), sum(22 * g.size for _, _, g in items)),
        name="adamw",
    )(*ins, *keep, *after)
    for n, (name, _, _) in enumerate(items):
        new[name] = got[3 * n : 3 * n + 3]
    return got[-1]


CHIPS = 8


def _fold_kernel(pos_ref, mine_ref, got_ref, *outs):
    chip, core = pos_ref[0], pos_ref[1]
    for delta, out in enumerate(outs):
        at = chip ^ delta
        out[...] = (mine_ref[core * CHIPS + at].astype(wide) + got_ref[at].astype(wide)).astype(low)


def fold(pos, g, got, after=()):
    shape = g.shape[1:]
    whole = lambda a: pl.BlockSpec(a.shape, lambda i, _: (0,) * a.ndim)
    return pl.pallas_call(
        _late(_fold_kernel, 3, len(after)),
        grid_spec=pltpu.PrefetchScalarGridSpec(num_scalar_prefetch=1, grid=(1,), in_specs=[whole(g), whole(got)] + [pl.BlockSpec(memory_space=pl.ANY)] * len(after),
                                               out_specs=[pl.BlockSpec(shape, lambda i, _: (0, 0))] * CHIPS),
        out_shape=[jax.ShapeDtypeStruct(shape, low)] * CHIPS,
        compiler_params=_params(),
        cost_estimate=_cost(2 * got.size, 8 * got.size),
        name="fold",
    )(pos, g, got, *after)


def swap_cores(x):
    return lax.ppermute(x, "dp", [(i, i ^ 1) for i in range(2 * CHIPS)])


def to_chip(x, delta):
    return lax.ppermute(x, "dp", [(i, i ^ (2 * delta)) for i in range(2 * CHIPS)])


def _sum_kernel(*refs):
    total = refs[0][...].astype(wide)
    for one in refs[1:-1]:
        total = total + one[...].astype(wide)
    refs[-1][...] = total.astype(low)


def _stack_kernel(*refs):
    for n, one in enumerate(refs[:-1]):
        refs[-1][n] = one[...]


def _joined(kernel, pieces, shape, after, name):
    n = len(pieces)
    return pl.pallas_call(
        _late(kernel, n, len(after)),
        grid=(1,),
        in_specs=[pl.BlockSpec(pieces[0].shape, lambda i: (0, 0))] * n + [pl.BlockSpec(memory_space=pl.ANY)] * len(after),
        out_specs=pl.BlockSpec(shape, lambda i: (0,) * len(shape)),
        out_shape=jax.ShapeDtypeStruct(shape, low),
        compiler_params=_params(),
        cost_estimate=_cost(1000, 4 * n * pieces[0].size),
        name=name,
    )(*pieces, *after)


def stack(pieces, after=()):
    return _joined(_stack_kernel, pieces, (len(pieces), *pieces[0].shape), after, "stack")


def sum_pieces(pieces, after=()):
    return _joined(_sum_kernel, pieces, pieces[0].shape, after, "sum")


def _adamw_q_kernel(pos_ref, *refs, kept, widths):
    ins, (a_ref, b_ref), outs = refs[: 3 * len(widths)], refs[3 * len(widths) : 3 * len(widths) + 2], refs[3 * len(widths) + 2 + kept :]
    outs[-1][...] = jnp.zeros_like(outs[-1])
    chip, core = pos_ref[0], pos_ref[1]
    first = lax.rem(chip, 2)
    here = lax.div(pl.program_id(0), CHIPS // 2) == core
    at = 0
    for n, width in enumerate(widths):
        cols = slice(at, at + width)
        at += width
        rows = [jnp.where(here, a_ref[x, :, cols].astype(wide), b_ref[x, :, cols].astype(wide)) for x in (first, 1 - first)]
        g = jnp.concatenate(rows, axis=0)
        w = ins[3 * n][...].astype(wide)
        m = 0.9 * ins[3 * n + 1][...] + 0.1 * g
        v = 0.95 * ins[3 * n + 2][...] + 0.05 * g * g
        outs[3 * n][...] = (w - 0.02 * (m * lax.rsqrt(v + 1e-8) + 0.1 * w)).astype(low)
        outs[3 * n + 1][...] = m
        outs[3 * n + 2][...] = v


def adamw_q(pos, names, number, own, other, state, new, after=()):
    ins, specs, shapes, keep, widths = [], [], [], [], []
    for name in names:
        w = state[name][0]
        rows, cols = w.shape[1:]
        widths.append(cols)
        spec = pl.BlockSpec((None, rows // CHIPS, cols), lambda i, _: (number, i, 0))
        for one in state[name]:
            ins.append(one)
            specs.append(spec)
            shapes.append(jax.ShapeDtypeStruct(one.shape, one.dtype))
        if name in new:
            keep += list(new[name])
    piece = pl.BlockSpec((2, *own.shape[1:]), lambda i, pos: (lax.rem(i, CHIPS // 2) ^ lax.div(pos[0], 2), 0, 0))
    got = pl.pallas_call(
        functools.partial(_adamw_q_kernel, kept=len(keep) + len(after), widths=widths),
        grid_spec=pltpu.PrefetchScalarGridSpec(
            num_scalar_prefetch=1, grid=(CHIPS,),
            in_specs=specs + [piece, piece] + [pl.BlockSpec(memory_space=pl.ANY)] * (len(keep) + len(after)),
            out_specs=specs + [pl.BlockSpec((8, HEAD), lambda i, _: (0, 0))]),
        out_shape=shapes + [jax.ShapeDtypeStruct((8, HEAD), wide)],
        input_output_aliases={1 + len(ins) + 2 + n: n for n in range(len(keep))},
        compiler_params=_params(),
        cost_estimate=_cost(4000 * own.size * 2, 44 * own.size),
        name="adamw_q",
    )(pos, *ins, own, other, *keep, *after)
    for n, name in enumerate(names):
        new[name] = got[3 * n : 3 * n + 3]
    return got[-1]


def solution(mesh):
    def step(x, dy, *arrays):
        weights, m, v = (arrays[i : i + 7] for i in (0, 7, 14))
        state = {name: one for name, *one in zip(NAMES, weights, m, v, strict=True)}
        wq, wk, wv, wo, wg, wu, wd = weights
        layers = wq.shape[0]
        h, by = x[0], dy[0]
        t, d = h.shape
        me = lax.axis_index("dp")
        chip, core = me // 2, me % 2
        pos = jnp.stack([chip, core]).astype(jnp.int32)
        half = HEAD // 2
        angle = jnp.arange(t, dtype=wide)[:, None] * THETA ** (-jnp.arange(half, dtype=wide) / half)
        cos, sin = jnp.cos(angle), jnp.sin(angle)
        cos, sin = jnp.concatenate([cos, cos], 1), jnp.concatenate([-sin, sin], 1)
        kept = []
        for n in range(layers):
            q, k, val = project(h, wq, wk, wv, cos, sin, n)
            att, lse = attend(q, k, val)
            if n < layers - 1:
                h1, h2 = post(att, h, wo, wg, wu, wd, n)
                kept.append((h, q, k, val, att, lse, h1))
                h = h2
            else:
                kept.append((h, q, k, val, att, lse, h))
        new, sums, last_sum = {}, {}, None
        moving = None
        for n in reversed(range(layers)):
            h, q, k, val, att, lse, h1 = kept[n]
            wait = (moving[3],) if moving else ()
            by1, datt, delta, *mine = post_bwd(att, h1, by, wo, wg, wu, wd, n, n == layers - 1, wait)
            mine = tuple(mine)
            if last_sum is not None:
                mine, _ = lax.optimization_barrier((mine, last_sum))
            sums[n] = last_sum = lax.psum(mine, "dp")
            wait = ()
            if moving:
                pieces = fold(pos, moving[1], moving[2], (delta,))
                arrived = [to_chip(pieces[i], i) for i in range(1, CHIPS)]
                wait = (pieces[0],)
            dq, dk, dv = attend_bwd(q, k, val, datt, lse, delta, wait)
            if moving:
                total = sum_pieces([pieces[0]] + arrived, (dk,))
                back = moving[0], [total] + [to_chip(total, i) for i in range(1, CHIPS)]
                wait = (total,)
            dw, *by = project_bwd(dq, dk, dv, h, cos, sin, n, n > 0, by1, wq, wk, wv, wait)
            by = by[0] if by else None
            dw = dw.reshape(2 * CHIPS, d // (2 * CHIPS), dw.shape[1])
            sent = lax.dynamic_slice_in_dim(dw, (1 - core) * CHIPS, CHIPS)
            moving = n, dw, swap_cores(sent), sent
        mlp, qkv = ("wo", "w_gate", "w_up", "w_down"), ("wq", "wk", "wv")
        one, zero = ([(name, n, g) for name, g in zip(mlp, sums[n])] for n in (1, 0))
        number, dw, got, sent = moving
        token = adamw(one[:2], state, new, (sent,))
        pieces, earlier = fold(pos, dw, got, (token,)), stack(back[1], (token,))
        arrived = [to_chip(pieces[i], i) for i in range(1, CHIPS)]
        swapped = swap_cores(earlier)
        token = adamw(one[2:], state, new, (pieces[0], earlier))
        total = sum_pieces([pieces[0]] + arrived, (token,))
        returned = [to_chip(total, i) for i in range(1, CHIPS)]
        token = adamw_q(pos, qkv, back[0], earlier, swapped, state, new, (total,))
        own = stack([total] + returned, (token,))
        swapped = swap_cores(own)
        token = adamw(zero, state, new, (own,))
        adamw_q(pos, qkv, number, own, swapped, state, new, (token,))
        return tuple(new[name][which] for which in range(3) for name in NAMES)

    states, all_of = P(("rep", "dp"), None, None), P(None, None, None)
    return jax.shard_map(
        step,
        mesh=mesh,
        in_specs=(states, states) + (all_of,) * 21,
        out_specs=(P("rep", None, None),) * 21,
        check_vma=False,
    )
```
